32 devices in a mesh: gx: 4 (over y, core), gy: 2 (over x), gz: 4 (over z).
Axes of the slice: x: 2, y: 2, z: 4, core: 2. Of those that a mesh axis runs over, the one named last changes fastest.
Arguments:
- source: float32 [256, 128, 128], P('gx', 'gy', 'gz'), may hold values from -6 to 6
- green: float32 [512, 256, 256], P(None, ('gx', 'gz'), 'gy'), may hold values from 0.05 to 2, as said below
Outputs:
- potential: float32 [256, 128, 128], P('gx', 'gy', 'gz')
The draws below stay inside these ranges and needn't reach their ends.
Inputs may be any that keep to these rules, and one draw needn't show every extreme that they name: `green`: greenfull is even: greenfull[k] equals greenfull at (-k1 mod 512, -k2 mod 256, -k3 mod 256).
All inputs are finite; a program needn't handle non-finite values.
Results may differ from the reference program's by a relative error of at most 0.00007.
Values sent between devices are 32-bit elements; how exact they have to be, the bound alone decides.
No kernel may reach another device: no remote copies, remote signals or barrier semaphores. Data moves between devices by JAX's collectives and lax.ppermute only.
A program may use at most 128 MiB of HBM per device.

```python
import math
import jax
import jax.numpy as jnp

NX = 256
NY = 128
NZ = 128
LX = 512
LY = 256
LZ = 256


def pair_frequency(length):
    position = jnp.arange(length, dtype=jnp.int32)
    unit_index = position // 2
    member = position % 2
    return jnp.where(unit_index == 0, member * (length // 2), jnp.where(member == 0, unit_index, length - unit_index)).astype(jnp.int32)


def draw_green(key, part):
    lower_end = 0.05
    upper_end = 2.0
    drawn = jnp.exp(jax.random.uniform(key, (LX, LY, LZ), jnp.float32, math.log(lower_end), math.log(upper_end)))
    mirrored = jnp.roll(jnp.flip(drawn, (0, 1, 2)), (1, 1, 1), (0, 1, 2))
    symmetric = 0.5 * (drawn + mirrored)
    ordered = jnp.take(symmetric, pair_frequency(LY), axis=1)
    return jnp.take(ordered, pair_frequency(LZ), axis=2)


def level_of(rng, shape, cuts, smallest, top_value):
    factor_of, own = 1.0, jax.random.fold_in(rng, 6)
    for axis_at, shards_of in cuts:
        heights = jnp.exp(jax.random.uniform(jax.random.fold_in(own, axis_at), (shards_of,), jnp.float32, smallest / len(cuts), top_value / len(cuts)))
        factor_of = factor_of * jnp.repeat(heights, shape[axis_at] // shards_of).reshape([-1 if axis == axis_at else 1 for axis in range(len(shape))])
    return factor_of


def centred(stream_key, shape, spread, bound, shards=(), kind=jnp.bfloat16):
    entries = spread * jax.random.normal(stream_key, shape, jnp.float32)
    if shards:
        entries = entries * level_of(stream_key, shape, shards, -0.22, 0.18)
    return jnp.clip(entries, -bound, bound).astype(kind)


def setup_inputs(seed: int = 0) -> dict:
    key_list = jax.random.split(jax.random.key(seed), 3)
    source = centred(key_list[0], (NX, NY, NZ), 1.0, 6.0, ((0, 4), (1, 2), (2, 4)), jnp.float32)
    green = draw_green(jax.random.fold_in(key_list[2], 71), 0)
    return {"source": source, "green": green}


def pair_position(length):
    freq = jnp.arange(length, dtype=jnp.int32)
    half = length // 2
    return jnp.where(freq == 0, 0, jnp.where(freq == half, 1, jnp.where(freq < half, 2 * freq, 2 * (length - freq) + 1))).astype(jnp.int32)


def reference(source, green):
    natural = jnp.take(green, pair_position(LY), axis=1)
    natural = jnp.take(natural, pair_position(LZ), axis=2)
    padded = jnp.pad(source, ((0, NX), (0, NY), (0, NZ)))
    spectrum = jnp.fft.fftn(padded)
    inverse = jnp.fft.ifftn(spectrum * natural)
    return jnp.real(inverse)[:NX, :NY, :NZ].astype(jnp.float32)
```

```python
import math

import jax
import jax.numpy as jnp
import numpy as np
from jax import lax
from jax.experimental import pallas as pl
from jax.experimental.pallas import tpu as pltpu
from jax.sharding import PartitionSpec as P

LANES = 128
SUBS = 8


def pair_frequency(length):
    position = np.arange(length)
    unit = position // 2
    member = position % 2
    return np.where(unit == 0, member * (length // 2), np.where(member == 0, unit, length - unit))


def trig(rows, cols, length):
    angles = (rows[:, None] * cols[None, :] % length) * (2.0 * math.pi / length)
    return np.cos(angles), np.sin(angles)


def split_table(table):
    table = np.asarray(table, np.float32)
    high = table.astype(jnp.bfloat16)
    low = (table - high.astype(np.float32)).astype(jnp.bfloat16)
    return jnp.asarray(high), jnp.asarray(low)


def halves(value):
    high = value.astype(jnp.bfloat16)
    low = (value - high.astype(jnp.float32)).astype(jnp.bfloat16)
    return high, low


def mm(a, b):
    dot = lambda p, q: jnp.dot(p, q, preferred_element_type=jnp.float32)
    return dot(a[0], b[0]) + (dot(a[0], b[1]) + dot(a[1], b[0]))


def call(body, out_shape, operands, scratch=(), specs=None):
    vmem = pl.BlockSpec(memory_space=pltpu.VMEM)
    return pl.pallas_call(
        body,
        out_shape=out_shape,
        in_specs=specs or [vmem] * len(operands),
        out_specs=jax.tree.map(lambda _: vmem, out_shape),
        scratch_shapes=list(scratch),
        compiler_params=pltpu.CompilerParams(vmem_limit_bytes=56 * 2**20),
    )(*operands)


def block_transpose(pieces, brick):
    count = len(pieces)
    lane = lax.broadcasted_iota(jnp.int32, pieces[0].shape, 1) // brick
    pieces = list(pieces)
    step = 1
    while step < count:
        odd = (lane // step) % 2 == 1
        for at in range(count):
            if (at // step) % 2 == 0:
                low, high = pieces[at], pieces[at + step]
                pieces[at] = jnp.where(odd, pltpu.roll(high, step * brick, 1), low)
                pieces[at + step] = jnp.where(
                    odd, high, pltpu.roll(low, LANES - step * brick, 1)
                )
        step *= 2
    return pieces


def per_device(source, green):
    size_gx = lax.axis_size("gx")
    size_gy = lax.axis_size("gy")
    size_gz = lax.axis_size("gz")
    brick_x, brick_y, brick_z = source.shape
    grid_x, grid_y, grid_z = brick_x * size_gx, brick_y * size_gy, brick_z * size_gz
    long_x, long_y, long_z = 2 * grid_x, 2 * grid_y, 2 * grid_z
    group = size_gx * size_gz
    part_x = brick_x // size_gy
    per_tile = LANES // brick_z
    tiles_x = part_x // per_tile
    tiles_z = grid_z // LANES
    rows_c = tiles_x * SUBS
    count_k = long_z // size_gy
    units = grid_y
    f32 = jnp.float32
    h = lax.axis_index("gy")
    first = (lax.axis_index("gx") * size_gz + lax.axis_index("gz") == 0).astype(jnp.int32)
    where = jnp.stack([h.astype(jnp.int32), first])
    smem = pl.BlockSpec(memory_space=pltpu.SMEM)
    vmem = pl.BlockSpec(memory_space=pltpu.VMEM)

    def shift(value, step):
        perm = [(i, (i + step) % size_gy) for i in range(size_gy)]
        return lax.ppermute(value, "gy", perm)

    def pack_body(where_ref, src_ref, *outs):
        for step in range(size_gy):
            base = (where_ref[0] + step) % size_gy * part_x
            for c in range(tiles_x):
                outs[step][:, c * LANES : (c + 1) * LANES] = jnp.concatenate(
                    [src_ref[base + c * per_tile + p] for p in range(per_tile)], axis=1
                )

    packed = call(
        pack_body,
        [jax.ShapeDtypeStruct((brick_y, tiles_x * LANES), f32)] * size_gy,
        (where, source),
        specs=[smem, vmem],
    )
    lines = [packed[0]] + [shift(packed[s], s) for s in range(1, size_gy)]

    sign_y = 1.0 - 2.0 * (np.arange(grid_y) % 2)
    cos_y, sin_y = trig(np.arange(units), np.arange(grid_y), long_y)
    im_y = -sin_y
    im_y[0] = sign_y
    fwd_y = np.concatenate([cos_y, im_y], 0)
    fwd_y = fwd_y.reshape(2 * units, size_gy, brick_y).transpose(1, 0, 2)
    fwd_y = split_table(fwd_y)

    def y_body(where_ref, high_ref, low_ref, *refs):
        ins, outs = refs[:size_gy], refs[size_gy:]
        total = None
        for s in range(size_gy):
            block = (where_ref[0] + size_gy - s) % size_gy
            term = mm((high_ref[block], low_ref[block]), halves(ins[s][...]))
            total = term if total is None else total + term
        for part in range(2):
            for c in range(tiles_x):
                piece = total[part * units : (part + 1) * units, c * LANES : (c + 1) * LANES]
                outs[part][:, c * SUBS : (c + 1) * SUBS, :] = piece.reshape(group, SUBS, LANES)

    plane = jax.ShapeDtypeStruct((group, rows_c, LANES), f32)
    spectra = call(
        y_body, [plane] * 2, (where, *fwd_y, *lines), specs=[smem] + [vmem] * (2 + size_gy)
    )

    def exchange(value):
        return lax.all_to_all(value, ("gx", "gz"), 0, 0, tiled=True)

    own = [exchange(v) for v in spectra]
    gathered = list(own)
    for s in range(1, size_gy):
        gathered += [shift(v, s) for v in own]

    freq_z = pair_frequency(long_z).reshape(size_gy, count_k)
    fwd_z, inv_z = [], []
    for block in range(size_gy):
        c, s = trig(np.arange(grid_z), freq_z[block], long_z)
        fwd_z.append(np.block([[c, -s], [s, c]]))
        inv_z.append(np.block([[c.T, s.T], [-s.T, c.T]]) / long_z)
    fwd_z = split_table(np.stack(fwd_z))
    inv_z = split_table(np.stack(inv_z))
    ih, ig, ip, ic = np.meshgrid(
        np.arange(size_gy), np.arange(size_gx), np.arange(per_tile), np.arange(tiles_x),
        indexing="ij",
    )
    order_x = (ig * brick_x + ih * part_x + ic * per_tile + ip).reshape(-1)
    cos_x, sin_x = trig(np.arange(grid_x), order_x, long_x)
    sin_x[0] = 1.0 - 2.0 * (order_x % 2)
    weight = np.where(np.arange(grid_x) == 0, 0.5, 1.0)[:, None] / long_x
    fwd_x = split_table(np.concatenate([cos_x, sin_x], 0))
    inv_x = split_table(np.concatenate([cos_x * weight, sin_x * weight], 0).T)
    own_rows = green.shape[1]
    green_rows = green.reshape(long_x * own_rows, count_k)
    block_rows = per_tile * rows_c

    def middle_body(where_ref, green_ref, edge_ref, fzh, fzl, izh, izl, fxh, fxl, ixh, ixl, *refs):
        ins = refs[: 2 * size_gy]
        outs = refs[2 * size_gy : 4 * size_gy]
        field = refs[4 * size_gy]
        here = where_ref[0]
        is_first = where_ref[1] == 1
        table_z = (fzh[here], fzl[here])
        back_z = (izh[here], izl[here])
        for s in range(size_gy):
            side = (here + size_gy - s) % size_gy
            for g in range(size_gx):
                cols = []
                for part in range(2):
                    ref = ins[2 * s + part]
                    for t in range(tiles_z):
                        at = g * size_gz + t * per_tile
                        cols.append(
                            jnp.concatenate(
                                block_transpose([ref[at + q] for q in range(per_tile)], brick_z), 0
                            )
                        )
                rows = jnp.concatenate(cols, 1)
                out = mm(halves(rows), table_z)
                offset = pl.multiple_of((side * size_gx + g) * block_rows, block_rows)
                field[pl.ds(offset, block_rows), :] = out[:, :count_k]
                field[pl.ds(size_rows + offset, block_rows), :] = out[:, count_k:]

        def mirror(value):
            lane = lax.broadcasted_iota(jnp.int32, value.shape, 1)
            swapped = jnp.where(
                lane % 2 == 0, pltpu.roll(value, count_k - 1, 1), pltpu.roll(value, 1, 1)
            )
            keep = jnp.logical_and(here == 0, lane < 2)
            return jnp.where(keep, value, swapped)

        def filtered(re, im, row_p, row_m):
            both = mm((fxh[...], fxl[...]), halves(jnp.concatenate([re, im], 1)))
            cr, ci = both[:grid_x, :count_k], both[:grid_x, count_k:]
            sr, si = both[grid_x:, :count_k], both[grid_x:, count_k:]
            gp = green_ref[pl.ds(row_p, grid_x, stride=own_rows), :]
            gm = mirror(green_ref[pl.ds(row_m, grid_x, stride=own_rows), :])
            ga, gb = gp + gm, gp - gm
            edge = edge_ref[pl.ds(row_p, 1), :] + mirror(edge_ref[pl.ds(row_m, 1), :])
            top = lax.broadcasted_iota(jnp.int32, ga.shape, 0) == 0
            gb = jnp.where(top, 0.0, gb)
            ge = jnp.where(top, edge, ga)
            even = jnp.concatenate([ga * cr + gb * si, ga * ci - gb * sr], 1)
            odd = jnp.concatenate([ge * sr - gb * ci, gb * cr + ge * si], 1)
            return mm((ixh[...], ixl[...]), halves(jnp.concatenate([even, odd], 0)))

        for u in range(SUBS):
            at_re = pl.ds(u, grid_x, stride=SUBS)
            at_im = pl.ds(size_rows + u, grid_x, stride=SUBS)
            if u == 0:

                @pl.when(is_first)
                def _():
                    re, im = field[at_re, :], field[at_im, :]
                    are = 0.5 * (re + mirror(re))
                    aim = 0.5 * (im - mirror(im))
                    out = filtered(are, aim, 0, 0) + filtered(re - are, im - aim, 1, 1)
                    field[at_re, :] = out[:, :count_k]
                    field[at_im, :] = out[:, count_k:]

                @pl.when(jnp.logical_not(is_first))
                def _():
                    out = filtered(field[at_re, :], field[at_im, :], 0, 1)
                    field[at_re, :] = out[:, :count_k]
                    field[at_im, :] = out[:, count_k:]
            else:
                out = filtered(field[at_re, :], field[at_im, :], 2 * u, 2 * u + 1)
                field[at_re, :] = out[:, :count_k]
                field[at_im, :] = out[:, count_k:]

        for s in range(size_gy):
            side = (here + size_gy - s) % size_gy
            for g in range(size_gx):
                offset = pl.multiple_of((side * size_gx + g) * block_rows, block_rows)
                rows = jnp.concatenate(
                    [
                        field[pl.ds(offset, block_rows), :],
                        field[pl.ds(size_rows + offset, block_rows), :],
                    ],
                    1,
                )
                out = mm(halves(rows), back_z)
                for part in range(2):
                    for t in range(tiles_z):
                        lo = (part * tiles_z + t) * LANES
                        col = out[:, lo : lo + LANES]
                        pieces = block_transpose(
                            [col[p * rows_c : (p + 1) * rows_c] for p in range(per_tile)], brick_z
                        )
                        for q in range(per_tile):
                            outs[2 * s + part][g * size_gz + t * per_tile + q] = pieces[q]

    size_rows = grid_x * SUBS
    operands = (where, green_rows, green_rows, *fwd_z, *inv_z, *fwd_x, *inv_x, *gathered)
    whole = lambda value: pl.BlockSpec(value.shape, lambda i: (0,) * value.ndim)
    returned = pl.pallas_call(
        middle_body,
        grid=(1,),
        out_shape=[plane] * (2 * size_gy),
        in_specs=[
            smem,
            pl.BlockSpec((grid_x * own_rows, count_k), lambda i: (0, 0)),
            pl.BlockSpec((own_rows, count_k), lambda i: (grid_x, 0)),
        ]
        + [whole(v) for v in operands[3:]],
        out_specs=[whole(plane)] * (2 * size_gy),
        scratch_shapes=[pltpu.VMEM((2 * size_rows, count_k), f32)],
        compiler_params=pltpu.CompilerParams(vmem_limit_bytes=56 * 2**20),
    )(*operands)
    summed = list(returned[:2])
    for s in range(1, size_gy):
        for part in range(2):
            summed[part] = summed[part] + shift(returned[2 * s + part], size_gy - s)
    last = [exchange(v) for v in summed]

    cos_b, sin_b = trig(np.arange(grid_y), np.arange(units), long_y)
    inv_re = 2.0 * cos_b
    inv_re[:, 0] = 1.0
    inv_im = -2.0 * sin_b
    inv_im[:, 0] = sign_y
    inv_y = np.concatenate([inv_re, inv_im], 1) / long_y
    inv_y = split_table(inv_y.reshape(size_gy, brick_y, 2 * units))

    def back_body(where_ref, high_ref, low_ref, re_ref, im_ref, *outs):
        rows = jnp.concatenate(
            [
                jnp.concatenate(
                    [
                        ref[:, c * SUBS : (c + 1) * SUBS, :].reshape(units, LANES)
                        for c in range(tiles_x)
                    ],
                    1,
                )
                for ref in (re_ref, im_ref)
            ],
            0,
        )
        rows = halves(rows)
        for s in range(size_gy):
            block = (where_ref[0] + s) % size_gy
            outs[s][...] = mm((high_ref[block], low_ref[block]), rows)

    lines = call(
        back_body,
        [jax.ShapeDtypeStruct((brick_y, tiles_x * LANES), f32)] * size_gy,
        (where, *inv_y, *last),
        specs=[smem] + [vmem] * 4,
    )
    lines = [lines[0]] + [shift(lines[s], s) for s in range(1, size_gy)]

    def unpack_body(where_ref, *refs):
        ins, out = refs[:size_gy], refs[size_gy]
        for s in range(size_gy):
            base = (where_ref[0] + size_gy - s) % size_gy * part_x
            for x in range(part_x):
                out[base + x] = ins[s][:, x * brick_z : (x + 1) * brick_z]

    return call(
        unpack_body,
        jax.ShapeDtypeStruct(source.shape, f32),
        (where, *lines),
        specs=[smem] + [vmem] * size_gy,
    )


def solution(mesh):
    return jax.shard_map(
        per_device,
        mesh=mesh,
        in_specs=(P("gx", "gy", "gz"), P(None, ("gx", "gz"), "gy")),
        out_specs=P("gx", "gy", "gz"),
        check_vma=False,
    )
```

```python
import functools
import math

import jax
import jax.numpy as jnp
import numpy as np
from jax import lax
from jax.experimental import pallas as pl
from jax.experimental.pallas import tpu as pltpu
from jax.sharding import PartitionSpec as P

LANES = 128
SUBS = 8
CHUNKS = 2


def pair_frequency(length):
    position = np.arange(length)
    unit = position // 2
    member = position % 2
    return np.where(unit == 0, member * (length // 2), np.where(member == 0, unit, length - unit))


def trig(rows, cols, length):
    angles = (rows[:, None] * cols[None, :] % length) * (2.0 * math.pi / length)
    return np.cos(angles), np.sin(angles)


def split_table(table):
    table = np.asarray(table, np.float32)
    high = table.astype(jnp.bfloat16)
    low = (table - high.astype(np.float32)).astype(jnp.bfloat16)
    return jnp.asarray(high), jnp.asarray(low)


def halves(value):
    high = value.astype(jnp.bfloat16)
    low = (value - high.astype(jnp.float32)).astype(jnp.bfloat16)
    return high, low


def mm(a, b):
    dot = lambda p, q: jnp.dot(p, q, preferred_element_type=jnp.float32)
    return dot(a[0], b[0]) + (dot(a[0], b[1]) + dot(a[1], b[0]))


def call(body, out_shape, operands, scratch=(), specs=None):
    vmem = pl.BlockSpec(memory_space=pltpu.VMEM)
    return pl.pallas_call(
        body,
        out_shape=out_shape,
        in_specs=specs or [vmem] * len(operands),
        out_specs=jax.tree.map(lambda _: vmem, out_shape),
        scratch_shapes=list(scratch),
        compiler_params=pltpu.CompilerParams(vmem_limit_bytes=56 * 2**20),
    )(*operands)


def block_transpose(pieces, brick):
    count = len(pieces)
    lane = lax.broadcasted_iota(jnp.int32, pieces[0].shape, 1) // brick
    pieces = list(pieces)
    step = 1
    while step < count:
        odd = (lane // step) % 2 == 1
        for at in range(count):
            if (at // step) % 2 == 0:
                low, high = pieces[at], pieces[at + step]
                pieces[at] = jnp.where(odd, pltpu.roll(high, step * brick, 1), low)
                pieces[at + step] = jnp.where(
                    odd, high, pltpu.roll(low, LANES - step * brick, 1)
                )
        step *= 2
    return pieces


def per_device(source, green):
    size_gx = lax.axis_size("gx")
    size_gy = lax.axis_size("gy")
    size_gz = lax.axis_size("gz")
    brick_x, brick_y, brick_z = source.shape
    grid_x, grid_y, grid_z = brick_x * size_gx, brick_y * size_gy, brick_z * size_gz
    long_x, long_y, long_z = 2 * grid_x, 2 * grid_y, 2 * grid_z
    group = size_gx * size_gz
    part_x = brick_x // size_gy
    per_tile = LANES // brick_z
    tiles_x = part_x // per_tile
    tiles_z = grid_z // LANES
    sub = SUBS // CHUNKS
    rows_c = tiles_x * sub
    count_k = long_z // size_gy
    units = grid_y
    f32 = jnp.float32
    h = lax.axis_index("gy")
    first = (lax.axis_index("gx") * size_gz + lax.axis_index("gz") == 0).astype(jnp.int32)
    where = jnp.stack([h.astype(jnp.int32), first])
    smem = pl.BlockSpec(memory_space=pltpu.SMEM)
    vmem = pl.BlockSpec(memory_space=pltpu.VMEM)

    def shift(value, step):
        perm = [(i, (i + step) % size_gy) for i in range(size_gy)]
        return lax.ppermute(value, "gy", perm)

    def pack_body(where_ref, src_ref, *outs):
        for step in range(size_gy):
            base = (where_ref[0] + step) % size_gy * part_x
            for c in range(tiles_x):
                piece = src_ref[pl.ds(base + c * per_tile, per_tile)]
                outs[step][:, c * LANES : (c + 1) * LANES] = piece.reshape(LANES, brick_y).T

    packed = call(
        pack_body,
        [jax.ShapeDtypeStruct((brick_y, tiles_x * LANES), f32)] * size_gy,
        (where, jnp.swapaxes(source, 1, 2)),
        specs=[smem, vmem],
    )
    lines = [packed[0]] + [shift(packed[s], s) for s in range(1, size_gy)]

    sign_y = 1.0 - 2.0 * (np.arange(grid_y) % 2)
    cos_y, sin_y = trig(np.arange(units), np.arange(grid_y), long_y)
    im_y = -sin_y
    im_y[0] = sign_y
    fwd_y = np.concatenate([cos_y, im_y], 0)
    fwd_y = fwd_y.reshape(2 * units, size_gy, brick_y).transpose(1, 0, 2)
    fwd_y = split_table(fwd_y)

    def y_body(where_ref, high_ref, low_ref, *refs):
        ins, outs = refs[:size_gy], refs[size_gy:]
        total = None
        for s in range(size_gy):
            block = (where_ref[0] + size_gy - s) % size_gy
            term = mm((high_ref[block], low_ref[block]), halves(ins[s][...]))
            total = term if total is None else total + term
        for part in range(2):
            for c in range(tiles_x):
                piece = total[part * units : (part + 1) * units, c * LANES : (c + 1) * LANES]
                piece = piece.reshape(group, SUBS, LANES)
                at = part * rows_c + c * sub
                for k in range(CHUNKS):
                    outs[k][:, at : at + sub, :] = piece[:, k * sub : (k + 1) * sub]

    plane = jax.ShapeDtypeStruct((group, 2 * rows_c, LANES), f32)
    spectra = call(
        y_body, [plane] * CHUNKS, (where, *fwd_y, *lines), specs=[smem] + [vmem] * (2 + size_gy)
    )

    def exchange(value):
        return lax.all_to_all(value, ("gx", "gz"), 0, 0, tiled=True)

    freq_z = pair_frequency(long_z).reshape(size_gy, count_k)
    fwd_z, inv_z = [], []
    for block in range(size_gy):
        c, s = trig(np.arange(grid_z), freq_z[block], long_z)
        fwd_z.append(np.block([[c, -s], [s, c]]))
        inv_z.append(np.block([[c.T, s.T], [-s.T, c.T]]) / long_z)
    fwd_z = split_table(np.stack(fwd_z))
    inv_z = split_table(np.stack(inv_z))
    ih, ig, ip, ic = np.meshgrid(
        np.arange(size_gy), np.arange(size_gx), np.arange(per_tile), np.arange(tiles_x),
        indexing="ij",
    )
    order_x = (ig * brick_x + ih * part_x + ic * per_tile + ip).reshape(-1)
    cos_x, sin_x = trig(np.arange(grid_x), order_x, long_x)
    sin_x[0] = 1.0 - 2.0 * (order_x % 2)
    weight = np.where(np.arange(grid_x) == 0, 0.5, 1.0)[:, None] / long_x
    fwd_x = split_table(np.concatenate([cos_x, sin_x], 0))
    inv_x = split_table(np.concatenate([cos_x * weight, sin_x * weight], 0).T)
    own_rows = green.shape[1]
    green_sub = own_rows // CHUNKS
    block_rows = per_tile * rows_c

    def middle_body(
        k, where_ref, green_ref, edge_ref, fzh, fzl, izh, izl, fxh, fxl, ixh, ixl, *refs
    ):
        ins = refs[:size_gy]
        outs = refs[size_gy : 2 * size_gy]
        field = refs[2 * size_gy]
        here = where_ref[0]
        is_first = where_ref[1] == 1
        table_z = (fzh[here], fzl[here])
        back_z = (izh[here], izl[here])
        for s in range(size_gy):
            side = (here + size_gy - s) % size_gy
            for g in range(size_gx):
                cols = []
                for part in range(2):
                    lo = part * rows_c
                    for t in range(tiles_z):
                        at = g * size_gz + t * per_tile
                        cols.append(
                            jnp.concatenate(
                                block_transpose([ins[s][at + q, lo : lo + rows_c] for q in range(per_tile)], brick_z), 0
                            )
                        )
                rows = jnp.concatenate(cols, 1)
                out = mm(halves(rows), table_z)
                offset = pl.multiple_of((side * size_gx + g) * block_rows, block_rows)
                field[pl.ds(offset, block_rows), :] = out[:, :count_k]
                field[pl.ds(size_rows + offset, block_rows), :] = out[:, count_k:]

        def mirror(value):
            lane = lax.broadcasted_iota(jnp.int32, value.shape, 1)
            swapped = jnp.where(
                lane % 2 == 0, pltpu.roll(value, count_k - 1, 1), pltpu.roll(value, 1, 1)
            )
            keep = jnp.logical_and(here == 0, lane < 2)
            return jnp.where(keep, value, swapped)

        def filtered(re, im, row_p, row_m):
            both = mm((fxh[...], fxl[...]), halves(jnp.concatenate([re, im], 1)))
            cr, ci = both[:grid_x, :count_k], both[:grid_x, count_k:]
            sr, si = both[grid_x:, :count_k], both[grid_x:, count_k:]
            gp = green_ref[:, row_p, :]
            gm = mirror(green_ref[:, row_m, :])
            ga, gb = gp + gm, gp - gm
            edge = edge_ref[0, row_p : row_p + 1, :] + mirror(edge_ref[0, row_m : row_m + 1, :])
            top = lax.broadcasted_iota(jnp.int32, ga.shape, 0) == 0
            gb = jnp.where(top, 0.0, gb)
            ge = jnp.where(top, edge, ga)
            even = jnp.concatenate([ga * cr + gb * si, ga * ci - gb * sr], 1)
            odd = jnp.concatenate([ge * sr - gb * ci, gb * cr + ge * si], 1)
            return mm((ixh[...], ixl[...]), halves(jnp.concatenate([even, odd], 0)))

        for u in range(sub):
            at_re = pl.ds(u, grid_x, stride=sub)
            at_im = pl.ds(size_rows + u, grid_x, stride=sub)
            if u == 0 and k == 0:

                @pl.when(is_first)
                def _():
                    re, im = field[at_re, :], field[at_im, :]
                    are = 0.5 * (re + mirror(re))
                    aim = 0.5 * (im - mirror(im))
                    out = filtered(are, aim, 0, 0) + filtered(re - are, im - aim, 1, 1)
                    field[at_re, :] = out[:, :count_k]
                    field[at_im, :] = out[:, count_k:]

                @pl.when(jnp.logical_not(is_first))
                def _():
                    out = filtered(field[at_re, :], field[at_im, :], 0, 1)
                    field[at_re, :] = out[:, :count_k]
                    field[at_im, :] = out[:, count_k:]
            else:
                out = filtered(field[at_re, :], field[at_im, :], 2 * u, 2 * u + 1)
                field[at_re, :] = out[:, :count_k]
                field[at_im, :] = out[:, count_k:]

        for s in range(size_gy):
            side = (here + size_gy - s) % size_gy
            for g in range(size_gx):
                offset = pl.multiple_of((side * size_gx + g) * block_rows, block_rows)
                rows = jnp.concatenate(
                    [
                        field[pl.ds(offset, block_rows), :],
                        field[pl.ds(size_rows + offset, block_rows), :],
                    ],
                    1,
                )
                out = mm(halves(rows), back_z)
                for part in range(2):
                    for t in range(tiles_z):
                        lo = (part * tiles_z + t) * LANES
                        col = out[:, lo : lo + LANES]
                        pieces = block_transpose(
                            [col[p * rows_c : (p + 1) * rows_c] for p in range(per_tile)], brick_z
                        )
                        for q in range(per_tile):
                            at = g * size_gz + t * per_tile + q
                            outs[s][at, part * rows_c : (part + 1) * rows_c] = pieces[q]

    size_rows = grid_x * sub
    whole = lambda value: pl.BlockSpec(value.shape, lambda i: (0,) * value.ndim)

    def middle(k, gathered):
        operands = (where, green, green, *fwd_z, *inv_z, *fwd_x, *inv_x, *gathered)
        return pl.pallas_call(
            functools.partial(middle_body, k),
            grid=(1,),
            out_shape=[plane] * size_gy,
            in_specs=[
                smem,
                pl.BlockSpec((grid_x, green_sub, count_k), lambda i: (0, k, 0)),
                pl.BlockSpec((1, green_sub, count_k), lambda i: (grid_x, k, 0)),
            ]
            + [whole(v) for v in operands[3:]],
            out_specs=[whole(plane)] * size_gy,
            scratch_shapes=[pltpu.VMEM((2 * size_rows, count_k), f32)],
            compiler_params=pltpu.CompilerParams(vmem_limit_bytes=40 * 2**20),
            name=f"middle{k}",
        )(*operands)

    last = []
    own = [exchange(v) for v in spectra]
    for k in range(CHUNKS):
        gathered = [own[k]] + [shift(own[k], s) for s in range(1, size_gy)]
        returned = middle(k, gathered)
        summed = returned[0]
        for s in range(1, size_gy):
            summed = summed + shift(returned[s], size_gy - s)
        last.append(exchange(summed))

    cos_b, sin_b = trig(np.arange(grid_y), np.arange(units), long_y)
    inv_re = 2.0 * cos_b
    inv_re[:, 0] = 1.0
    inv_im = -2.0 * sin_b
    inv_im[:, 0] = sign_y
    inv_y = np.concatenate([inv_re, inv_im], 1) / long_y
    inv_y = split_table(inv_y.reshape(size_gy, brick_y, 2 * units))

    def back_body(where_ref, high_ref, low_ref, *refs):
        ins, outs = refs[:CHUNKS], refs[CHUNKS:]
        cols = []
        for c in range(tiles_x):
            pieces = []
            for part in range(2):
                at = part * rows_c + c * sub
                piece = jnp.concatenate([ref[:, at : at + sub, :] for ref in ins], 1)
                pieces.append(piece.reshape(units, LANES))
            cols.append(jnp.concatenate(pieces, 0))
        rows = jnp.concatenate(cols, 1)
        rows = halves(rows)
        for s in range(size_gy):
            block = (where_ref[0] + s) % size_gy
            outs[s][...] = mm((high_ref[block], low_ref[block]), rows)

    lines = call(
        back_body,
        [jax.ShapeDtypeStruct((brick_y, tiles_x * LANES), f32)] * size_gy,
        (where, *inv_y, *last),
        specs=[smem] + [vmem] * (2 + CHUNKS),
    )
    lines = [lines[0]] + [shift(lines[s], s) for s in range(1, size_gy)]

    def unpack_body(where_ref, *refs):
        ins, out = refs[:size_gy], refs[size_gy]
        for s in range(size_gy):
            base = (where_ref[0] + size_gy - s) % size_gy * part_x
            for c in range(tiles_x):
                piece = ins[s][:, c * LANES : (c + 1) * LANES].T
                out[pl.ds(base + c * per_tile, per_tile)] = piece.reshape(
                    per_tile, brick_z, brick_y
                )

    result = call(
        unpack_body,
        jax.ShapeDtypeStruct((brick_x, brick_z, brick_y), f32),
        (where, *lines),
        specs=[smem] + [vmem] * size_gy,
    )
    return jnp.swapaxes(result, 1, 2)


def solution(mesh):
    return jax.shard_map(
        per_device,
        mesh=mesh,
        in_specs=(P("gx", "gy", "gz"), P(None, ("gx", "gz"), "gy")),
        out_specs=P("gx", "gy", "gz"),
        check_vma=False,
    )
```

```python
import functools
import math

import jax
import jax.numpy as jnp
import numpy as np
from jax import lax
from jax.experimental import pallas as pl
from jax.experimental.pallas import tpu as pltpu
from jax.sharding import PartitionSpec as P

LANES = 128
SUBS = 8
CHUNKS = 2


def pair_frequency(length):
    position = np.arange(length)
    unit = position // 2
    member = position % 2
    return np.where(unit == 0, member * (length // 2), np.where(member == 0, unit, length - unit))


def trig(rows, cols, length):
    angles = (rows[:, None] * cols[None, :] % length) * (2.0 * math.pi / length)
    return np.cos(angles), np.sin(angles)


def split_table(table):
    table = np.asarray(table, np.float32)
    high = table.astype(jnp.bfloat16)
    low = (table - high.astype(np.float32)).astype(jnp.bfloat16)
    return high, low


def halves(value):
    high = value.astype(jnp.bfloat16)
    low = (value - high.astype(jnp.float32)).astype(jnp.bfloat16)
    return high, low


def mm(a, b):
    dot = lambda p, q: jnp.dot(p, q, preferred_element_type=jnp.float32)
    return dot(a[0], b[0]) + (dot(a[0], b[1]) + dot(a[1], b[0]))


def call(body, out_shape, operands, scratch=(), specs=None):
    vmem = pl.BlockSpec(memory_space=pltpu.VMEM)
    return pl.pallas_call(
        body,
        out_shape=out_shape,
        in_specs=specs or [vmem] * len(operands),
        out_specs=jax.tree.map(lambda _: vmem, out_shape),
        scratch_shapes=list(scratch),
        compiler_params=pltpu.CompilerParams(vmem_limit_bytes=40 * 2**20),
    )(*operands)


def block_transpose(pieces, brick):
    count = len(pieces)
    lane = lax.broadcasted_iota(jnp.int32, pieces[0].shape, 1) // brick
    pieces = list(pieces)
    step = 1
    while step < count:
        odd = (lane // step) % 2 == 1
        for at in range(count):
            if (at // step) % 2 == 0:
                low, high = pieces[at], pieces[at + step]
                pieces[at] = jnp.where(odd, pltpu.roll(high, step * brick, 1), low)
                pieces[at + step] = jnp.where(
                    odd, high, pltpu.roll(low, LANES - step * brick, 1)
                )
        step *= 2
    return pieces


def per_device(source, green):
    size_gx = lax.axis_size("gx")
    size_gy = lax.axis_size("gy")
    size_gz = lax.axis_size("gz")
    brick_x, brick_y, brick_z = source.shape
    grid_x, grid_y, grid_z = brick_x * size_gx, brick_y * size_gy, brick_z * size_gz
    long_x, long_y, long_z = 2 * grid_x, 2 * grid_y, 2 * grid_z
    group = size_gx * size_gz
    part_x = brick_x // size_gy
    per_tile = LANES // brick_z
    tiles_x = part_x // per_tile
    tiles_z = grid_z // LANES
    sub = SUBS // CHUNKS
    rows_c = tiles_x * sub
    count_k = long_z // size_gy
    units = grid_y
    f32 = jnp.float32
    h = lax.axis_index("gy")
    first = (lax.axis_index("gx") * size_gz + lax.axis_index("gz") == 0).astype(jnp.int32)
    where = jnp.stack([h.astype(jnp.int32), first])
    smem = pl.BlockSpec(memory_space=pltpu.SMEM)
    vmem = pl.BlockSpec(memory_space=pltpu.VMEM)

    def shift(value, step):
        perm = [(i, (i + step) % size_gy) for i in range(size_gy)]
        return lax.ppermute(value, "gy", perm)

    def pack_body(where_ref, src_ref, *outs):
        for step in range(size_gy):
            base = (where_ref[0] + step) % size_gy * part_x
            for c in range(tiles_x):
                piece = src_ref[pl.ds(base + c * per_tile, per_tile)]
                outs[step][:, c * LANES : (c + 1) * LANES] = piece.reshape(LANES, brick_y).T

    packed = call(
        pack_body,
        [jax.ShapeDtypeStruct((brick_y, tiles_x * LANES), f32)] * size_gy,
        (where, jnp.swapaxes(source, 1, 2)),
        specs=[smem, vmem],
    )
    lines = [packed[0]] + [shift(packed[s], s) for s in range(1, size_gy)]

    sign_y = 1.0 - 2.0 * (np.arange(grid_y) % 2)
    cos_y, sin_y = trig(np.arange(units), np.arange(grid_y), long_y)
    im_y = -sin_y
    im_y[0] = sign_y
    fwd_y = np.concatenate([cos_y, im_y], 0)
    fwd_y = fwd_y.reshape(2 * units, size_gy, brick_y).transpose(1, 0, 2)
    fwd_y = [jnp.asarray(v) for v in split_table(fwd_y)]

    def y_body(where_ref, high_ref, low_ref, *refs):
        ins, outs = refs[:size_gy], refs[size_gy:]
        total = None
        for s in range(size_gy):
            block = (where_ref[0] + size_gy - s) % size_gy
            term = mm((high_ref[block], low_ref[block]), halves(ins[s][...]))
            total = term if total is None else total + term
        for part in range(2):
            for c in range(tiles_x):
                piece = total[part * units : (part + 1) * units, c * LANES : (c + 1) * LANES]
                piece = piece.reshape(group, SUBS, LANES)
                at = part * rows_c + c * sub
                for k in range(CHUNKS):
                    outs[k][:, at : at + sub, :] = piece[:, k * sub : (k + 1) * sub]

    plane = jax.ShapeDtypeStruct((group, 2 * rows_c, LANES), f32)
    spectra = call(
        y_body, [plane] * CHUNKS, (where, *fwd_y, *lines), specs=[smem] + [vmem] * (2 + size_gy)
    )

    def exchange(value):
        return lax.all_to_all(value, ("gx", "gz"), 0, 0, tiled=True)

    freq_z = pair_frequency(long_z).reshape(size_gy, count_k)
    fwd_z, inv_z = [], []
    for block in range(size_gy):
        c, s = trig(np.arange(grid_z), freq_z[block], long_z)
        fwd_z.append(np.block([[c, -s], [s, c]]))
        inv_z.append(np.block([[c.T, s.T], [-s.T, c.T]]) / long_z)
    fwd_z = split_table(np.stack(fwd_z))
    inv_z = split_table(np.stack(inv_z))
    ih, ig, ip, ic = np.meshgrid(
        np.arange(size_gy), np.arange(size_gx), np.arange(per_tile), np.arange(tiles_x),
        indexing="ij",
    )
    order_x = (ig * brick_x + ih * part_x + ic * per_tile + ip).reshape(-1)
    cos_x, sin_x = trig(np.arange(grid_x), order_x, long_x)
    sin_x[0] = 1.0 - 2.0 * (order_x % 2)
    weight = np.where(np.arange(grid_x) == 0, 0.5, 1.0)[:, None] / long_x
    fwd_x = split_table(np.concatenate([cos_x, sin_x], 0))
    inv_x = split_table(np.concatenate([cos_x * weight, sin_x * weight], 0).T)
    own_rows = green.shape[1]
    green_sub = own_rows // CHUNKS
    block_rows = per_tile * rows_c

    width = 2 * LANES
    pieces, starts, at_row = [], {}, 0
    for name, pair in (("fz", fwd_z), ("iz", inv_z), ("fx", fwd_x), ("ix", inv_x)):
        for level in range(2):
            value = pair[level]
            value = value.reshape((-1,) + value.shape[-2:])
            starts[name, level] = (at_row, value.shape[1], value.shape[2] // width)
            for block in range(value.shape[0]):
                for col in range(0, value.shape[2], width):
                    pieces.append(value[block, :, col : col + width])
                    at_row += value.shape[1]
    tables = jnp.asarray(np.concatenate(pieces, 0))

    def middle_body(k, where_ref, green_hbm, table_ref, *refs):
        ins = refs[:size_gy]
        outs = refs[size_gy : 2 * size_gy]
        field, green_ref, edge_ref, sems = refs[2 * size_gy :]
        part_k = pl.ds(k * green_sub, green_sub)
        copies = [
            pltpu.make_async_copy(
                green_hbm.at[pl.ds(0, grid_x), part_k, :], green_ref, sems.at[0]
            ),
            pltpu.make_async_copy(
                green_hbm.at[pl.ds(grid_x, 1), part_k, :], edge_ref, sems.at[1]
            ),
        ]
        for copy in copies:
            copy.start()

        def table(name, block=0):
            levels = []
            for level in range(2):
                start, rows, cols = starts[name, level]
                base = start + block * (rows * cols)
                if not isinstance(block, int):
                    base = pl.multiple_of(base, 2 * SUBS)
                parts = [table_ref[pl.ds(base + c * rows, rows), :] for c in range(cols)]
                levels.append(parts[0] if cols == 1 else jnp.concatenate(parts, 1))
            return levels

        here = where_ref[0]
        is_first = where_ref[1] == 1
        table_z = table("fz", here)
        for s in range(size_gy):
            side = (here + size_gy - s) % size_gy
            for g in range(size_gx):
                cols = []
                for part in range(2):
                    lo = part * rows_c
                    for t in range(tiles_z):
                        at = g * size_gz + t * per_tile
                        cols.append(
                            jnp.concatenate(
                                block_transpose([ins[s][at + q, lo : lo + rows_c] for q in range(per_tile)], brick_z), 0
                            )
                        )
                rows = jnp.concatenate(cols, 1)
                out = mm(halves(rows), table_z)
                offset = pl.multiple_of((side * size_gx + g) * block_rows, block_rows)
                field[pl.ds(offset, block_rows), :] = out[:, :count_k]
                field[pl.ds(size_rows + offset, block_rows), :] = out[:, count_k:]

        for copy in copies:
            copy.wait()

        def mirror(value):
            lane = lax.broadcasted_iota(jnp.int32, value.shape, 1)
            swapped = jnp.where(
                lane % 2 == 0, pltpu.roll(value, count_k - 1, 1), pltpu.roll(value, 1, 1)
            )
            keep = jnp.logical_and(here == 0, lane < 2)
            return jnp.where(keep, value, swapped)

        def filtered(re, im, row_p, row_m):
            both = mm(table("fx"), halves(jnp.concatenate([re, im], 1)))
            cr, ci = both[:grid_x, :count_k], both[:grid_x, count_k:]
            sr, si = both[grid_x:, :count_k], both[grid_x:, count_k:]
            gp = green_ref[:, row_p, :]
            gm = mirror(green_ref[:, row_m, :])
            ga, gb = gp + gm, gp - gm
            edge = edge_ref[0, row_p : row_p + 1, :] + mirror(edge_ref[0, row_m : row_m + 1, :])
            top = lax.broadcasted_iota(jnp.int32, ga.shape, 0) == 0
            gb = jnp.where(top, 0.0, gb)
            ge = jnp.where(top, edge, ga)
            even = jnp.concatenate([ga * cr + gb * si, ga * ci - gb * sr], 1)
            odd = jnp.concatenate([ge * sr - gb * ci, gb * cr + ge * si], 1)
            return mm(table("ix"), halves(jnp.concatenate([even, odd], 0)))

        for u in range(sub):
            at_re = pl.ds(u, grid_x, stride=sub)
            at_im = pl.ds(size_rows + u, grid_x, stride=sub)
            if u == 0 and k == 0:

                @pl.when(is_first)
                def _():
                    re, im = field[at_re, :], field[at_im, :]
                    are = 0.5 * (re + mirror(re))
                    aim = 0.5 * (im - mirror(im))
                    out = filtered(are, aim, 0, 0) + filtered(re - are, im - aim, 1, 1)
                    field[at_re, :] = out[:, :count_k]
                    field[at_im, :] = out[:, count_k:]

                @pl.when(jnp.logical_not(is_first))
                def _():
                    out = filtered(field[at_re, :], field[at_im, :], 0, 1)
                    field[at_re, :] = out[:, :count_k]
                    field[at_im, :] = out[:, count_k:]
            else:
                out = filtered(field[at_re, :], field[at_im, :], 2 * u, 2 * u + 1)
                field[at_re, :] = out[:, :count_k]
                field[at_im, :] = out[:, count_k:]

        back_z = table("iz", here)
        for s in range(size_gy):
            side = (here + size_gy - s) % size_gy
            for g in range(size_gx):
                offset = pl.multiple_of((side * size_gx + g) * block_rows, block_rows)
                rows = jnp.concatenate(
                    [
                        field[pl.ds(offset, block_rows), :],
                        field[pl.ds(size_rows + offset, block_rows), :],
                    ],
                    1,
                )
                out = mm(halves(rows), back_z)
                for part in range(2):
                    for t in range(tiles_z):
                        lo = (part * tiles_z + t) * LANES
                        col = out[:, lo : lo + LANES]
                        pieces = block_transpose(
                            [col[p * rows_c : (p + 1) * rows_c] for p in range(per_tile)], brick_z
                        )
                        for q in range(per_tile):
                            at = g * size_gz + t * per_tile + q
                            outs[s][at, part * rows_c : (part + 1) * rows_c] = pieces[q]

    size_rows = grid_x * sub
    hbm = pl.BlockSpec(memory_space=pltpu.HBM)
    def middle(k, gathered):
        return call(
            functools.partial(middle_body, k),
            [plane] * size_gy,
            (where, green, tables, *gathered),
            scratch=[
                pltpu.VMEM((2 * size_rows, count_k), f32),
                pltpu.VMEM((grid_x, green_sub, count_k), f32),
                pltpu.VMEM((1, green_sub, count_k), f32),
                pltpu.SemaphoreType.DMA((2,)),
            ],
            specs=[smem, hbm, vmem] + [vmem] * size_gy,
        )

    last = []
    own = [exchange(v) for v in spectra]
    for k in range(CHUNKS):
        gathered = [own[k]] + [shift(own[k], s) for s in range(1, size_gy)]
        returned = middle(k, gathered)
        summed = returned[0]
        for s in range(1, size_gy):
            summed = summed + shift(returned[s], size_gy - s)
        last.append(exchange(summed))

    cos_b, sin_b = trig(np.arange(grid_y), np.arange(units), long_y)
    inv_re = 2.0 * cos_b
    inv_re[:, 0] = 1.0
    inv_im = -2.0 * sin_b
    inv_im[:, 0] = sign_y
    inv_y = np.concatenate([inv_re, inv_im], 1) / long_y
    inv_y = split_table(inv_y.reshape(size_gy, brick_y, 2 * units))
    inv_y = [jnp.asarray(v) for v in inv_y]

    def back_body(where_ref, high_ref, low_ref, *refs):
        ins, outs = refs[:CHUNKS], refs[CHUNKS:]
        cols = []
        for c in range(tiles_x):
            pieces = []
            for part in range(2):
                at = part * rows_c + c * sub
                piece = jnp.concatenate([ref[:, at : at + sub, :] for ref in ins], 1)
                pieces.append(piece.reshape(units, LANES))
            cols.append(jnp.concatenate(pieces, 0))
        rows = jnp.concatenate(cols, 1)
        rows = halves(rows)
        for s in range(size_gy):
            block = (where_ref[0] + s) % size_gy
            outs[s][...] = mm((high_ref[block], low_ref[block]), rows)

    lines = call(
        back_body,
        [jax.ShapeDtypeStruct((brick_y, tiles_x * LANES), f32)] * size_gy,
        (where, *inv_y, *last),
        specs=[smem] + [vmem] * (2 + CHUNKS),
    )
    lines = [lines[0]] + [shift(lines[s], s) for s in range(1, size_gy)]

    def unpack_body(where_ref, *refs):
        ins, out = refs[:size_gy], refs[size_gy]
        for s in range(size_gy):
            base = (where_ref[0] + size_gy - s) % size_gy * part_x
            for c in range(tiles_x):
                piece = ins[s][:, c * LANES : (c + 1) * LANES].T
                out[pl.ds(base + c * per_tile, per_tile)] = piece.reshape(
                    per_tile, brick_z, brick_y
                )

    result = call(
        unpack_body,
        jax.ShapeDtypeStruct((brick_x, brick_z, brick_y), f32),
        (where, *lines),
        specs=[smem] + [vmem] * size_gy,
    )
    return jnp.swapaxes(result, 1, 2)


def solution(mesh):
    return jax.shard_map(
        per_device,
        mesh=mesh,
        in_specs=(P("gx", "gy", "gz"), P(None, ("gx", "gz"), "gy")),
        out_specs=P("gx", "gy", "gz"),
        check_vma=False,
    )
```
